32 devices in a mesh: dp: 4 (over z), stage: 2 (over y), tp: 4 (over x, core).
Axes of the slice: x: 2, y: 2, z: 4, core: 2. Of those that a mesh axis runs over, the one named last changes fastest.
Arguments:
- act_mb1: bfloat16 [2, 16, 14, 14, 512], P('stage', ('dp', 'tp'))
- act_mb2: bfloat16 [2, 16, 14, 14, 512], P('stage', ('dp', 'tp'))
- conv_w: bfloat16 [2, 3, 3, 512, 512], P('stage', None, None, 'tp')
- gamma_scale: float32 [2, 512], P('stage', 'tp')
- beta_shift: float32 [2, 512], P('stage', 'tp')
- dz_mb1: bfloat16 [2, 16, 14, 14, 512], P('stage', 'dp', None, None, 'tp')
- dz_mb2: bfloat16 [2, 16, 14, 14, 512], P('stage', 'dp', None, None, 'tp')
Outputs:
- output 1: bfloat16 [2, 16, 14, 14, 512], P('stage', 'dp', None, None, 'tp')
- output 2: bfloat16 [2, 16, 14, 14, 512], P('stage', 'dp', None, None, 'tp')
- output 3: bfloat16 [2, 16, 14, 14, 512], P('stage', ('dp', 'tp'))
- output 4: bfloat16 [2, 16, 14, 14, 512], P('stage', ('dp', 'tp'))
- output 5: float32 [2, 3, 3, 512, 512], P('stage', None, None, 'tp')
All inputs are finite; a program needn't handle non-finite values.
Results may differ from the reference program's by a relative error of at most 0.00363.
Values are sent between devices in bfloat16 or wider.
A program may use at most 1 GiB of HBM per device.

```python
import jax
import jax.numpy as jnp
from jax import lax

STAGES = 2
BLOCKS = 16
IMG_DEV = 1
SIDE_LEN = 14
IN_CHANNELS = 512
OUT_CHANNELS = 512

BATCH = BLOCKS * IMG_DEV


def stage_slot(values, slot):
    mask = (jnp.arange(STAGES) == slot).astype(values.dtype)
    return mask.reshape((STAGES,) + (1,) * values.ndim) * values[None]


def setup_inputs(seed: int = 0) -> dict:
    key_list = jax.random.split(jax.random.key(seed), 7)
    act_shape = (BATCH, SIDE_LEN, SIDE_LEN, IN_CHANNELS)
    out_shape = (BATCH, SIDE_LEN, SIDE_LEN, OUT_CHANNELS)
    fan_scale = (9 * IN_CHANNELS) ** -0.5
    act_mb1 = stage_slot(jax.random.normal(key_list[0], act_shape, jnp.float32), 0).astype(jnp.bfloat16)
    act_mb2 = stage_slot(jax.random.normal(key_list[1], act_shape, jnp.float32), 0).astype(jnp.bfloat16)
    conv_w = stage_slot(jax.random.normal(key_list[2], (3, 3, IN_CHANNELS, OUT_CHANNELS), jnp.float32) * fan_scale, 1).astype(jnp.bfloat16)
    gamma_scale = stage_slot(1.0 + 0.3 * jax.random.normal(key_list[3], (OUT_CHANNELS,), jnp.float32), 1)
    beta_shift = stage_slot(0.5 * jax.random.normal(key_list[4], (OUT_CHANNELS,), jnp.float32), 1)
    dz_mb1 = stage_slot(jax.random.normal(key_list[5], out_shape, jnp.float32), 1).astype(jnp.bfloat16)
    dz_mb2 = stage_slot(jax.random.normal(key_list[6], out_shape, jnp.float32), 1).astype(jnp.bfloat16)
    return {'act_mb1': act_mb1, 'act_mb2': act_mb2, 'conv_w': conv_w, 'gamma_scale': gamma_scale, 'beta_shift': beta_shift, 'dz_mb1': dz_mb1, 'dz_mb2': dz_mb2}


def conv_f32(act_in, kernel):
    return lax.conv_general_dilated(act_in, kernel, (1, 1), 'SAME', dimension_numbers=('NHWC', 'HWIO', 'NHWC'))


def micro_pass(act_all, dz_all, kernel, gain_vec, shift_vec):
    kernel_f = kernel.astype(jnp.float32)
    act_blocks = act_all.reshape((BLOCKS, IMG_DEV) + act_all.shape[1:])
    dz_blocks = dz_all.reshape((BLOCKS, IMG_DEV) + dz_all.shape[1:])

    def block_step(dw_acc, block_pair):
        act_blk, dz_blk = block_pair
        pre_act, conv_vjp = jax.vjp(conv_f32, act_blk.astype(jnp.float32), kernel_f)
        y_lin = pre_act * gain_vec + shift_vec
        z_blk = jnp.maximum(y_lin, 0.0).astype(jnp.bfloat16)
        g_blk = jnp.where(y_lin > 0, dz_blk.astype(jnp.float32) * gain_vec, 0.0).astype(jnp.bfloat16)
        d_act, d_kernel = conv_vjp(g_blk.astype(jnp.float32))
        return dw_acc + d_kernel, (z_blk, d_act.astype(jnp.bfloat16))

    dw_start = jnp.zeros(kernel.shape, jnp.float32)
    dw_total, (z_blocks, dact_blocks) = lax.scan(block_step, dw_start, (act_blocks, dz_blocks))
    return z_blocks.reshape(dz_all.shape), dact_blocks.reshape(act_all.shape), dw_total


def reference(act_mb1, act_mb2, conv_w, gamma_scale, beta_shift, dz_mb1, dz_mb2):
    kernel = conv_w[1]
    gain_vec = gamma_scale[1]
    shift_vec = beta_shift[1]
    z_one, dact_one, dw_one = micro_pass(act_mb1[0], dz_mb1[1], kernel, gain_vec, shift_vec)
    z_two, dact_two, dw_two = micro_pass(act_mb2[0], dz_mb2[1], kernel, gain_vec, shift_vec)
    return (stage_slot(z_one, 1), stage_slot(z_two, 1), stage_slot(dact_one, 0), stage_slot(dact_two, 0), stage_slot(dw_one + dw_two, 1))
```

```python
import functools

import jax
import jax.numpy as jnp
from jax import lax
from jax.experimental import pallas as pl
from jax.experimental.pallas import tpu as pltpu
from jax.sharding import PartitionSpec as P

MESH = pl.DeviceIdType.MESH
BF = jnp.bfloat16
F32 = jnp.float32

SIDE = 14
LW = 16
NI = 4
IL = 15
ML = NI * IL
PL = 66
TL = 64
MR = ML * LW
DENSE = NI * SIDE * SIDE


def row_target(idx):
    h = (idx * 1171) >> 16
    rem = idx - h * 56
    w = rem >> 2
    n = rem & 3
    return n * (IL * LW) + h * LW + w


def kernel(act1, act2, conv_w, gamma, beta, dz1, dz2,
           z1, z2, da1, da2, dw,
           kbuf, kown, arx, aoth, apad, dzv, dpad, zpad, pmat, grx, gpad, at3, dsend,
           ksend, krecv, kloc, lsem, asend, arecv, afwd, osend, orecv,
           gzs, gxs, gss, gfs, grecv, dsem, drecv):
    dp = lax.axis_index("dp")
    st = lax.axis_index("stage")
    tp = lax.axis_index("tp")
    sib = tp + 1 - 2 * (tp % 2)
    xnb = (tp + 2) % 4
    xsib = (sib + 2) % 4
    acts = (act1, act2)
    dzs = (dz1, dz2)
    zs = (z1, z2)
    das = (da1, da2)

    def remote(src, dst, ss, rs, dev):
        return pltpu.make_async_remote_copy(src_ref=src, dst_ref=dst, send_sem=ss, recv_sem=rs,
                                            device_id=dev, device_id_type=MESH)

    def lane(i):
        return pl.ds(pl.multiple_of(i * 128, 128), 128)

    def own_a(mb, slot, dev):
        return remote(acts[mb].at[0, 0], arx.at[mb, tp], asend.at[mb, slot], arecv.at[mb, tp], dev)

    def oth_a(mb, j, c):
        return remote(acts[mb].at[0, 0, :, :, pl.ds(c * 128, 128)], aoth.at[mb, dp, tp],
                      osend.at[mb, j, c], orecv.at[mb, dp, tp], ((dp + j) % 4, 1, c))

    barrier = pltpu.get_barrier_semaphore()

    @pl.when(st == 0)
    def _():
        def hello(i, _):
            pl.semaphore_signal(barrier, inc=1, device_id=(i // 4, 1, i % 4), device_id_type=MESH)
            return 0
        lax.fori_loop(0, 16, hello, 0)
        pl.semaphore_wait(barrier, 16)
        for mb in range(2):
            own_a(mb, 0, (dp, 1, tp)).start()
            own_a(mb, 1, (dp, 1, xnb)).start()
        for mb in range(2):
            zs[mb][...] = jnp.zeros(z1.shape, BF)
        dw[...] = jnp.zeros(dw.shape, F32)
        for mb in range(2):
            own_a(mb, 0, (dp, 1, tp)).wait_send()
            own_a(mb, 1, (dp, 1, xnb)).wait_send()
        for mb in range(2):
            for j in range(1, 4):
                for c in range(4):
                    oth_a(mb, j, c).start()
        for mb in range(2):
            for j in range(1, 4):
                for c in range(4):
                    oth_a(mb, j, c).wait_send()
        for mb in range(2):
            for c in range(4):
                remote(dsend.at[mb, 0], das[mb].at[:, :, pl.ds(c * 128, 128)], dsem.at[mb, c],
                       drecv.at[mb, c], (dp, 1, c)).wait_recv()

    @pl.when(st == 1)
    def _():
        def hello(i, _):
            pl.semaphore_signal(barrier, inc=1, device_id=(i // 4, 0, i % 4), device_id_type=MESH)
            return 0
        lax.fori_loop(0, 16, hello, 0)
        for j in range(1, 4):
            pl.semaphore_signal(barrier, inc=1, device_id=((dp + j) % 4, 1, tp), device_id_type=MESH)
            pl.semaphore_signal(barrier, inc=1, device_id=(dp, 1, (tp + j) % 4), device_id_type=MESH)
        pl.semaphore_wait(barrier, 22)

        def k_copy(j, kw):
            c = (tp + j) % 4
            return remote(conv_w.at[0, :, kw, :, lane(c)],
                          kbuf.at[:, lane(tp), pl.ds(kw * 128, 128)],
                          ksend.at[c, kw], krecv.at[tp, kw], (dp, 1, c))

        def k_wait(j, kw):
            c = (tp + j) % 4
            return remote(conv_w.at[0, :, kw, :, lane(c)],
                          kbuf.at[:, lane(c), pl.ds(kw * 128, 128)],
                          ksend.at[c, kw], krecv.at[c, kw], (dp, 1, c))

        def k_local(kw):
            return pltpu.make_async_copy(conv_w.at[0, :, kw, :, lane(tp)],
                                         kbuf.at[:, lane(tp), pl.ds(kw * 128, 128)], kloc.at[kw])

        for j in (2, 3, 1):
            for kw in range(3):
                k_copy(j, kw).start()
        for kw in range(3):
            k_local(kw).start()
        own_k = pltpu.make_async_copy(conv_w.at[0], kown, lsem.at[0])
        own_k.start()
        for mb in range(2):
            pltpu.make_async_copy(dzs[mb], dzv.at[mb], lsem.at[1 + mb]).start()

        for mb in range(2):
            das[mb][...] = jnp.zeros(da1.shape, BF)
        dw[...] = jnp.zeros(dw.shape, F32)
        apad[...] = jnp.zeros(apad.shape, BF)
        gpad[...] = jnp.zeros(gpad.shape, BF)

        def place(rows, cols, fixed):
            a = lax.broadcasted_iota(jnp.int32, (rows, cols), 0)
            b = lax.broadcasted_iota(jnp.int32, (rows, cols), 1)
            hit = (row_target(b) == a) if fixed else (row_target(a) == b)
            return jnp.where(hit, 1.0, 0.0).astype(BF)

        for r in range(4):
            rows = MR // 4
            a = lax.broadcasted_iota(jnp.int32, (rows, DENSE), 0) + r * rows
            b = row_target(lax.broadcasted_iota(jnp.int32, (1, DENSE), 1))
            pmat[r * rows:(r + 1) * rows, :DENSE] = jnp.where(a == b, 1.0, 0.0).astype(BF)
        for mb in range(2):
            pltpu.make_async_copy(dzs[mb], dzv.at[mb], lsem.at[1 + mb]).wait()
            for r in range(4):
                rows = MR // 4
                dpad[mb, r * rows:(r + 1) * rows, :] = jnp.dot(
                    pmat[r * rows:(r + 1) * rows, :DENSE], dzv[mb],
                    preferred_element_type=F32).astype(BF)
        for r in range(7):
            rows = DENSE // 7
            a = row_target(lax.broadcasted_iota(jnp.int32, (rows, 1), 0) + r * rows)
            b = lax.broadcasted_iota(jnp.int32, (rows, MR), 1)
            pmat[r * rows:(r + 1) * rows, :MR] = jnp.where(a == b, 1.0, 0.0).astype(BF)
        own_k.wait()

        def g_slot(mb, d, t):
            return grx.at[mb, d, t]

        def g_z(mb, j):
            return remote(g_slot(mb, dp, tp), g_slot(mb, dp, tp), gzs.at[mb, j], grecv.at[mb, dp, tp],
                          ((dp + j) % 4, 1, tp))

        def g_x(mb, d):
            return remote(g_slot(mb, d, tp), g_slot(mb, d, tp), gxs.at[mb, d], grecv.at[mb, d, tp],
                          (dp, 1, xnb))

        def g_s(mb, d):
            return remote(g_slot(mb, d, tp), g_slot(mb, d, tp), gss.at[mb, d], grecv.at[mb, d, tp],
                          (dp, 1, sib))

        def g_f(mb, d):
            return remote(g_slot(mb, d, xnb), g_slot(mb, d, xnb), gfs.at[mb, d], grecv.at[mb, d, xnb],
                          (dp, 1, sib))

        def g_wait(mb, d, t):
            remote(g_slot(mb, d, t), g_slot(mb, d, t), gss.at[mb, d], grecv.at[mb, d, t],
                   (dp, 1, sib)).wait_recv()

        def a_fwd(mb, t):
            return remote(arx.at[mb, t], arx.at[mb, t], afwd.at[mb, t], arecv.at[mb, t], (dp, 1, sib))

        def a_wait(mb, t):
            remote(arx.at[mb, t], arx.at[mb, t], afwd.at[mb, t], arecv.at[mb, t],
                   (dp, 1, sib)).wait_recv()

        def spread_g(mb, d):
            def line(i, _):
                n = i // SIDE
                l = 1 + n * IL + (i - n * SIDE)
                for t in range(4):
                    gpad[l, 0:SIDE, t * 128:(t + 1) * 128] = grx[mb, d, t, i]
                return 0
            lax.fori_loop(0, NI * SIDE, line, 0)

        def d_out(mb, i):
            return remote(dsend.at[mb, i], das0.at[mb] if False else (da1, da2)[0], dsem.at[mb, i],
                          drecv.at[mb, tp], (dp, 0, i))

        for mb in range(2):
            a_wait(mb, tp)
            a_fwd(mb, tp).start()
            a_wait(mb, xnb)
            a_fwd(mb, xnb).start()
            a_wait(mb, sib)
            a_wait(mb, xsib)
            for n in range(NI):
                def line(h, _):
                    apad[1 + n * IL + h, 0:SIDE, :] = arx[mb, n, h]
                    return 0
                lax.fori_loop(0, SIDE, line, 0)
            if mb == 0:
                for kw in range(3):
                    k_local(kw).wait()
                for j in (2, 3, 1):
                    for kw in range(3):
                        k_wait(j, kw).wait_recv()

            def forward(i, _):
                lhs = jnp.concatenate([apad[pl.ds(30 * i + kh, 30)].reshape(480, 512) for kh in range(3)], axis=1)
                part = jnp.dot(lhs, kbuf[...].reshape(1536, 384), preferred_element_type=F32)
                pre = pltpu.roll(part[:, 0:128], 1, 0) + part[:, 128:256] + pltpu.roll(part[:, 256:384], 479, 0)
                gain = gamma[...]
                y = pre * gain + beta[...]
                rows = pl.ds(pl.multiple_of(480 * i, 480), 480)
                zpad[rows, :] = jnp.maximum(y, 0.0).astype(BF)
                dval = dpad[mb, rows, :].astype(F32)
                g = jnp.where(y > 0, dval * gain, 0.0).astype(BF).reshape(30, LW, 128)
                for k in range(30):
                    n, h = divmod(k, IL)
                    if h < SIDE:
                        grx[mb, dp, tp, (2 * i + n) * SIDE + h] = g[k, 0:SIDE, :]
                return 0
            lax.fori_loop(0, 2, forward, 0)
            g_x(mb, dp).start()
            g_s(mb, dp).start()
            for j in (1, 3, 2):
                g_z(mb, j).start()
            for r in range(7):
                rows = DENSE // 7
                zs[mb][r * rows:(r + 1) * rows, :] = jnp.dot(
                    pmat[r * rows:(r + 1) * rows, :MR], zpad[...], preferred_element_type=F32).astype(BF)
            g_wait(mb, dp, xnb)
            g_f(mb, dp).start()
            if mb == 1:
                for j in (1, 3, 2):
                    d = (dp + j) % 4
                    g_wait(0, d, tp)
                    g_x(0, d).start()
                    g_s(0, d).start()
            g_wait(mb, dp, sib)
            g_wait(mb, dp, xsib)
            spread_g(mb, dp)

            def backward(i, _):
                lhs = jnp.concatenate([gpad[pl.ds(30 * i + 2 - kh, 30)].reshape(480, 512) for kh in range(3)], axis=1)
                rhs = jnp.concatenate([kown[kh].reshape(384, 512) for kh in range(3)], axis=1)
                part = lax.dot_general(lhs, rhs, (((1,), (1,)), ((), ())), preferred_element_type=F32)
                da = pltpu.roll(part[:, 0:128], 479, 0) + part[:, 128:256] + pltpu.roll(part[:, 256:384], 1, 0)
                da = da.astype(BF).reshape(30, LW, 128)
                for k in range(30):
                    n, h = divmod(k, IL)
                    if h < SIDE:
                        dsend[mb, 2 * i + n, h] = da[k, 0:SIDE, :]
                return 0
            lax.fori_loop(0, 2, backward, 0)
            for i in range(NI):
                remote(dsend.at[mb, i], das[mb].at[:, :, lane(tp)], dsem.at[mb, i], drecv.at[mb, tp],
                       (dp, 0, i)).start()

        def chunk(q, _):
            mb = q // 4
            j = q % 4
            d = (dp + j) % 4

            @pl.when(j > 0)
            def _():
                @pl.when(mb == 1)
                def _():
                    g_wait(1, d, tp)
                    g_x(1, d).start()
                    g_s(1, d).start()
                g_wait(mb, d, xnb)
                g_f(mb, d).start()
                g_wait(mb, d, sib)
                g_wait(mb, d, xsib)
                for n in range(NI):
                    remote(aoth.at[mb, d, n], aoth.at[mb, d, n], afwd.at[0, 0], orecv.at[mb, d, n],
                           (dp, 1, sib)).wait_recv()

                def line(i, _):
                    n = i // SIDE
                    apad[1 + n * IL + (i - n * SIDE), 0:SIDE, 0:128] = aoth[mb, d, n, i - n * SIDE]
                    return 0
                lax.fori_loop(0, NI * SIDE, line, 0)

            @pl.when(j == 0)
            def _():
                def line(i, _):
                    n = i // SIDE
                    apad[1 + n * IL + (i - n * SIDE), 0:SIDE, 0:128] = arx[mb, n, i - n * SIDE, :, lane(tp)]
                    return 0
                lax.fori_loop(0, NI * SIDE, line, 0)
            spread_g(mb, d)
            a = apad[1:1 + TL, :, 0:128].reshape(TL * LW, 128).astype(F32)
            at3[0:128, :] = pltpu.roll(a, 1, 0).T.astype(BF)
            at3[128:256, :] = a.T.astype(BF)
            at3[256:384, :] = pltpu.roll(a, TL * LW - 1, 0).T.astype(BF)
            for kh in range(3):
                dw[kh] += jnp.dot(at3[...], gpad[2 - kh:2 - kh + TL].reshape(TL * LW, 512),
                                  preferred_element_type=F32)
            return 0
        lax.fori_loop(0, 8, chunk, 0)

        for j in (2, 3, 1):
            for kw in range(3):
                k_copy(j, kw).wait_send()
        for mb in range(2):
            a_fwd(mb, tp).wait_send()
            a_fwd(mb, xnb).wait_send()
            for j in range(1, 4):
                g_z(mb, j).wait_send()
            for d in range(4):
                g_x(mb, d).wait_send()
                g_s(mb, d).wait_send()
                g_f(mb, d).wait_send()
            for i in range(NI):
                remote(dsend.at[mb, i], das[mb].at[:, :, lane(tp)], dsem.at[mb, i], drecv.at[mb, tp],
                       (dp, 0, i)).wait_send()


def solution(mesh):
    act_spec = P('stage', ('dp', 'tp'), None, None, None)
    w_spec = P('stage', None, None, 'tp', None)
    vec_spec = P('stage', 'tp')
    dz_spec = P('stage', 'dp', None, None, 'tp')
    hbm = pl.BlockSpec(memory_space=pl.ANY)
    vmem = pl.BlockSpec(memory_space=pltpu.VMEM)
    dma = pltpu.SemaphoreType.DMA

    def dense(dz):
        return dz[0].transpose(1, 2, 0, 3).reshape(DENSE, 128)

    def undense(z):
        return z.reshape(SIDE, SIDE, NI, 128).transpose(2, 0, 1, 3)[None]

    def device_body(act_mb1, act_mb2, conv_w, gamma_scale, beta_shift, dz_mb1, dz_mb2):
        z1, z2, da1, da2, dw = pl.pallas_call(
            kernel,
            out_shape=(
                jax.ShapeDtypeStruct((DENSE, 128), BF),
                jax.ShapeDtypeStruct((DENSE, 128), BF),
                jax.ShapeDtypeStruct((SIDE, SIDE, 512), BF),
                jax.ShapeDtypeStruct((SIDE, SIDE, 512), BF),
                jax.ShapeDtypeStruct((3, 384, 512), F32),
            ),
            in_specs=[hbm, hbm, hbm, vmem, vmem, hbm, hbm],
            out_specs=(vmem,) * 5,
            scratch_shapes=[
                pltpu.VMEM((3, 512, 384), BF),
                pltpu.VMEM((3, 3, 128, 512), BF),
                pltpu.VMEM((2, 4, SIDE, SIDE, 512), BF),
                pltpu.VMEM((2, 4, 4, SIDE, SIDE, 128), BF),
                pltpu.VMEM((PL, LW, 512), BF),
                pltpu.VMEM((2, DENSE, 128), BF),
                pltpu.VMEM((2, MR, 128), BF),
                pltpu.VMEM((MR, 128), BF),
                pltpu.VMEM((MR, 1024), BF),
                pltpu.VMEM((2, 4, 4, NI * SIDE, SIDE, 128), BF),
                pltpu.VMEM((PL, LW, 512), BF),
                pltpu.VMEM((384, TL * LW), BF),
                pltpu.VMEM((2, NI, SIDE, SIDE, 128), BF),
                dma((4, 3)), dma((4, 3)), dma((3,)), dma((3,)),
                dma((2, 2)), dma((2, 4)), dma((2, 4)), dma((2, 4, 4)), dma((2, 4, 4)),
                dma((2, 4)), dma((2, 4)), dma((2, 4)), dma((2, 4)), dma((2, 4, 4)),
                dma((2, 4)), dma((2, 4)),
            ],
            compiler_params=pltpu.CompilerParams(
                collective_id=0, has_side_effects=True, vmem_limit_bytes=60 * 1024 * 1024),
        )(act_mb1, act_mb2, conv_w, gamma_scale, beta_shift, dense(dz_mb1), dense(dz_mb2))
        return (undense(z1), undense(z2), da1[None, None], da2[None, None], dw.reshape(1, 3, 3, 128, 512))

    return jax.shard_map(device_body, mesh=mesh, in_specs=(act_spec, act_spec, w_spec, vec_spec, vec_spec, dz_spec, dz_spec), out_specs=(dz_spec, dz_spec, act_spec, act_spec, w_spec), check_vma=False)
```
